32 devices in a mesh: groups: 2 (over x), hst: 8 (over z, y), head: 2 (over core).
Axes of the slice: x: 2, y: 2, z: 4, core: 2. Of those that a mesh axis runs over, the one named last changes fastest.
Arguments:
- ctx_query: bfloat16 [3072, 64, 128], P(('groups', 'hst'), 'head'), parts along dimension 0, may hold values from -8 to 8
- ctx_key: bfloat16 [3072, 64, 128], P(('groups', 'hst'), 'head'), parts along dimension 0, may hold values from -8 to 8
- ctx_value: bfloat16 [3072, 64, 128], P(('groups', 'hst'), 'head'), parts along dimension 0, may hold values from -6 to 6
- valid: int32 [16], P(('groups', 'hst')), parts along dimension 0, may hold values from 128 to 192
- tail_query: bfloat16 [128, 64, 128], P(('groups', 'hst'), 'head'), parts along dimension 0, may hold values from -8 to 8
- tail_position: int32 [128], P(('groups', 'hst')), parts along dimension 0, may hold values from 1 to 1536
Outputs:
- ctx_out: bfloat16 [3072, 64, 128], P(('groups', 'hst'), 'head'), parts along dimension 0
- tail_out: bfloat16 [128, 64, 128], P(('groups', 'hst'), 'head'), parts along dimension 0
The draws below stay inside these ranges and needn't reach their ends.
There are 2 independent parts, one for each index of `groups`. The reference program is written for one: setup_inputs(seed, part) draws one part's arguments, and reference() takes and returns one part's arrays. A program takes and returns all parts, laid end to end along the dimension named above; each array names one. Nothing has to cross between parts.
All inputs are finite; a program needn't handle non-finite values.
Results may differ from the reference program's by a relative error of at most 0.0043.
Values may be sent and summed in bfloat16 or wider, within the bound.
A program may use at most 128 MiB of HBM per device.

```python
import jax
import jax.numpy as jnp
from jax import lax

HEADS = 64
HD = 128
BLOCK = 192
ANCHOR = 128
ROWS = 64
CONTEXT = 1536
N_HST = 8


def draw_ctx_key(key, part):
    base = jnp.clip(jax.random.normal(jax.random.fold_in(key, 202), (CONTEXT, HEADS, HD), jnp.float32), -4.0, 4.0)
    return base.astype(jnp.bfloat16)


def draw_ctx_query(key, part):
    base = jnp.clip(jax.random.normal(jax.random.fold_in(key, 303), (CONTEXT, HEADS, HD), jnp.float32), -4.0, 4.0)
    return base.astype(jnp.bfloat16)


def draw_tail_query(key, part):
    base = jnp.clip(jax.random.normal(jax.random.fold_in(key, 404), (ROWS, HEADS, HD), jnp.float32), -4.0, 4.0)
    return base.astype(jnp.bfloat16)


def plant(result, stream_key, least, high):
    spot = [jax.random.randint(jax.random.fold_in(stream_key, axis), (), 0, length) for axis, length in enumerate(result.shape)]
    longest = result.shape.index(max(result.shape))
    next_to = spot[:longest] + [(spot[longest] + 1) % result.shape[longest]] + spot[longest + 1:]
    return result.at[tuple(spot)].set(least).at[tuple(next_to)].set(high)


def block_scale(own_key, dims, shards, low, top_value):
    def one(position, parts):
        heights = jax.random.uniform(jax.random.fold_in(jax.random.fold_in(own_key, 6), position), (parts,), jnp.float32, low / len(shards), top_value / len(shards))
        return jnp.repeat(jnp.exp(heights), dims[position] // parts).reshape((-1,) + (1,) * (len(dims) - position - 1))

    gain = one(*shards[0])
    for cut in shards[1:]:
        gain = gain * one(*cut)
    return gain


def bell_draw(own_key, dims, deviation, limit, cuts=(), kind=jnp.bfloat16):
    values = deviation * jax.random.normal(own_key, dims, jnp.float32)
    if cuts:
        values = values * block_scale(own_key, dims, cuts, -0.22, 0.18)
    return jnp.clip(values, -limit, limit).astype(kind)


def setup_inputs(seed: int = 0, part: int = 0) -> dict:
    seeds = jax.random.split(jax.random.key(seed), 7)
    own_keys = jax.random.split(jax.random.fold_in(seeds[6], part), 7)
    return {
        "ctx_query": draw_ctx_query(jax.random.fold_in(jax.random.fold_in(seeds[6], part), 71), part),
        "ctx_key": draw_ctx_key(jax.random.fold_in(jax.random.fold_in(seeds[6], part), 71), part),
        "ctx_value": bell_draw(own_keys[2], (CONTEXT, HEADS, HD), 1.0, 6.0, ((0, 8), (1, 2))),
        "valid": plant(jax.random.randint(own_keys[3], (N_HST,), ANCHOR, BLOCK + 1), jax.random.fold_in(own_keys[3], 1), ANCHOR, BLOCK).astype(jnp.int32),
        "tail_query": draw_tail_query(jax.random.fold_in(jax.random.fold_in(seeds[6], part), 71), part),
        "tail_position": plant(jax.random.randint(own_keys[5], (ROWS,), 1, CONTEXT + 1), jax.random.fold_in(own_keys[5], 1), 1, CONTEXT).astype(jnp.int32),
    }


def first_phase(host, query, key, value, count, anchor_key, anchor_value):
    keys = jnp.concatenate([anchor_key, key], 0).astype(jnp.float32)
    values = jnp.concatenate([anchor_value, value], 0).astype(jnp.float32)
    rows = jnp.arange(BLOCK)[:, None]
    cols = jnp.arange(BLOCK)[None, :]
    own_mask = (cols <= rows) & (cols < count)
    anchor_mask = jnp.broadcast_to(host != 0, (BLOCK, ANCHOR))
    mask = jnp.concatenate([anchor_mask, own_mask], 1)
    scores = jnp.einsum('qhd,khd->hqk', query.astype(jnp.float32), keys) / jnp.sqrt(jnp.float32(HD))
    scores = jnp.where(mask[None], scores, jnp.float32(-1e+30))
    peak = lax.optimization_barrier(jnp.max(scores, axis=-1, keepdims=True))
    weights = jnp.where(mask[None], jnp.exp(scores - peak), jnp.float32(0.0))
    total = lax.optimization_barrier(jnp.sum(weights, axis=-1))
    rounded = weights.astype(jnp.bfloat16).astype(jnp.float32)
    summed = jnp.einsum('hqk,khd->qhd', rounded, values)
    return (summed / jnp.transpose(total)[:, :, None]).astype(jnp.bfloat16)

def reference(ctx_query, ctx_key, ctx_value, valid, tail_query, tail_position):
    anchor_key = ctx_key[:ANCHOR]
    anchor_value = ctx_value[:ANCHOR]
    shaped = (HEADS, HD)
    query_blocks = ctx_query.reshape((N_HST, BLOCK) + shaped)
    key_blocks = ctx_key.reshape((N_HST, BLOCK) + shaped)
    value_blocks = ctx_value.reshape((N_HST, BLOCK) + shaped)

    def one_block(items):
        host, query, key, value, count = items
        return first_phase(host, query, key, value, count, anchor_key, anchor_value)
    hosts = jnp.arange(N_HST).astype(jnp.int32)
    ctx_out = lax.map(one_block, (hosts, query_blocks, key_blocks, value_blocks, valid))
    ctx_out = ctx_out.reshape((N_HST * BLOCK,) + shaped)
    starts = (jnp.cumsum(valid) - valid).astype(jnp.int32)
    slots = jnp.arange(BLOCK).astype(jnp.int32)
    positions = (starts[:, None] + slots[None, :]).reshape(-1)
    live = (slots[None, :] < valid[:, None]).reshape(-1)
    mask = live[None, :] & (positions[None, :] < tail_position[:, None])
    scores = jnp.einsum('rhd,khd->hrk', tail_query.astype(jnp.float32), ctx_key.astype(jnp.float32)) / jnp.sqrt(jnp.float32(HD))
    scores = jnp.where(mask[None], scores, jnp.float32(-1e+30))
    peak = lax.optimization_barrier(jnp.max(scores, axis=-1, keepdims=True))
    weights = jnp.where(mask[None], jnp.exp(scores - peak), jnp.float32(0.0))
    total = lax.optimization_barrier(jnp.sum(weights, axis=-1))
    summed = jnp.einsum('hrk,khd->rhd', weights, ctx_value.astype(jnp.float32), precision=lax.Precision.HIGHEST)
    tail_out = (summed / jnp.transpose(total)[:, :, None]).astype(jnp.bfloat16)
    return (ctx_out, tail_out)
```

```python
import functools
import math

import jax
import jax.numpy as jnp
from jax import lax
from jax.experimental import pallas as pl
from jax.experimental.pallas import tpu as pltpu
from jax.sharding import PartitionSpec as P

ANCHOR = 128
GROUP = 8
PARTS = 4
NEG = -1e30
MESH = pl.DeviceIdType.MESH


def kernel(
    hosts, block, heads, rows, q_hbm, k_hbm, v_hbm, tq_hbm, info_hbm, out_hbm, tail_ref,
    q_raw, k_raw, v_raw, a_raw, qh, kh, vh, oh, o_raw, qbuf, ibuf, qt, bias, tbias, stat_m, stat_l,
    psend, precv, ssend, srecv, acc,
    load_sem, root_sem, own_sem, out_sem, a_recv, a_send, q_recv, i_recv, q_send, i_send,
    p_recv, s_recv, p_send, s_send,
):
    depth = hosts // 2
    groups = heads // GROUP
    half = groups // 2
    piece_rows = ANCHOR // PARTS
    pieces = half * 2 * PARTS
    per = 2 * PARTS
    total_rows = hosts * rows
    scale = math.log2(math.e) / math.sqrt(q_hbm.shape[-1])
    me = lax.axis_index("hst")
    z, y = me // 2, lax.rem(me, 2)
    root = me == 0

    def remote(src, dst, ssem, rsem, host):
        return pltpu.make_async_remote_copy(
            src_ref=src, dst_ref=dst, send_sem=ssem, recv_sem=rsem,
            device_id={"hst": host}, device_id_type=MESH,
        )

    def loads():
        for i, (hbm, raw) in enumerate(((k_hbm, k_raw), (v_hbm, v_raw), (q_hbm, q_raw))):
            for g in range(groups):
                yield pltpu.make_async_copy(
                    hbm.at[:, pl.ds(g * GROUP, GROUP), :], raw.at[g], load_sem.at[i, g]
                )

    def root_loads():
        for t in range(2):
            for p in range(pieces):
                hbm = k_hbm if (p // PARTS) % 2 == 0 else v_hbm
                g = t * half + p // per
                yield pltpu.make_async_copy(
                    hbm.at[pl.ds((p % PARTS) * piece_rows, piece_rows), pl.ds(g * GROUP, GROUP), :],
                    a_raw.at[t, p], root_sem.at[t, p],
                )

    def own_loads():
        yield pltpu.make_async_copy(tq_hbm, qbuf.at[me], own_sem.at[0])
        yield pltpu.make_async_copy(info_hbm, ibuf.at[me], own_sem.at[1])

    @pl.when(root)
    def _():
        for c in root_loads():
            c.start()

    for c in own_loads():
        c.start()
    for c in loads():
        c.start()

    barrier = pltpu.get_barrier_semaphore()

    def greet(k, _):
        pl.semaphore_signal(
            barrier, inc=1, device_id={"hst": lax.rem(me + k, hosts)}, device_id_type=MESH
        )
        return 0

    lax.fori_loop(1, hosts, greet, 0)
    pl.semaphore_wait(barrier, hosts - 1)

    def q_first(k):
        if k == 0:
            return z * 2 + 1 - y
        return lax.rem(z + k, depth) * 2 + y

    def q_copies(k):
        host = q_first(k)
        return (
            remote(tq_hbm, qbuf.at[me], q_send.at[k], q_recv.at[me], host),
            remote(info_hbm, ibuf.at[me], i_send.at[k], i_recv.at[me], host),
        )

    def q_forward(k):
        slot = lax.rem(z + depth - k, depth) * 2 + y
        host = z * 2 + 1 - y
        return (
            remote(qbuf.at[slot], qbuf.at[slot], q_send.at[depth - 1 + k], q_recv.at[slot], host),
            remote(ibuf.at[slot], ibuf.at[slot], i_send.at[depth - 1 + k], i_recv.at[slot], host),
        )

    def q_wait(slot):
        remote(qbuf.at[slot], qbuf.at[slot], q_send.at[0], q_recv.at[slot], me).wait_recv()
        remote(ibuf.at[slot], ibuf.at[slot], i_send.at[0], i_recv.at[slot], me).wait_recv()

    for k in range(depth):
        for c in q_copies(k):
            c.start()

    def sends(t, p):
        main = 1 - t
        ahead = (y == main) & (z + 1 < depth)
        cross = (y == main) & (z >= 1)
        out = [
            (ahead, a_send.at[t, 0, p], (z + 1) * 2 + main),
            (cross, a_send.at[t, 1, p], z * 2 + 1 - main),
        ]
        if t == 0:
            out.append((root, a_send.at[t, 1, p], 1))
        else:
            out.append(((y == 1) & (z == 1), a_send.at[t, 0, p], 1))
        for cond, sem, host in out:
            yield cond, remote(a_raw.at[t, p], a_raw.at[t, p], sem, a_recv.at[t, p], host)

    def forward(p):
        for t in range(2):
            for cond, copy in sends(t, p):
                @pl.when(cond)
                def _():
                    copy.start()

    def arrive(p):
        @pl.when(jnp.logical_not(root))
        def _():
            for t in range(2):
                remote(
                    a_raw.at[t, p], a_raw.at[t, p], a_send.at[t, 0, p], a_recv.at[t, p], me
                ).wait_recv()
                for cond, copy in sends(t, p):
                    @pl.when(cond)
                    def _():
                        copy.start()

    @pl.when(root)
    def _():
        for c in root_loads():
            c.wait()

        def body(p, _):
            for t in range(2):
                for cond, copy in sends(t, p):
                    @pl.when(cond)
                    def _():
                        copy.start()
            return 0

        lax.fori_loop(0, pieces, body, 0)

    for c in loads():
        c.wait()

    def relayout(g, _):
        at = pl.ds(g * GROUP, GROUP)
        kh[at, pl.ds(ANCHOR, block), :] = jnp.swapaxes(k_raw[g], 0, 1)
        vh[at, pl.ds(ANCHOR, block), :] = jnp.swapaxes(v_raw[g], 0, 1)
        qh[at] = jnp.swapaxes(q_raw[g], 0, 1)
        return 0

    lax.fori_loop(0, groups, relayout, 0)

    for c in own_loads():
        c.wait()
    count = ibuf[me][0:1, 0:1]
    keys = ANCHOR + block
    row = lax.broadcasted_iota(jnp.int32, (block, keys), 0)
    col = lax.broadcasted_iota(jnp.int32, (block, keys), 1)
    slot = col - ANCHOR
    own_bias = jnp.where((slot <= row) & (slot < count), jnp.float32(0.0), jnp.float32(NEG))
    bias[...] = jnp.where(slot < 0, jnp.where(root, jnp.float32(NEG), jnp.float32(0.0)), own_bias)

    for k in range(1, depth):
        q_wait(lax.rem(z + depth - k, depth) * 2 + y)
        for c in q_forward(k):
            c.start()
    for k in range(depth):
        q_wait(k * 2 + 1 - y)

    start = jnp.zeros((1, 1), jnp.int32)
    for s in range(hosts):
        start = start + ibuf[s][0:1, 0:1] * jnp.where(s < me, 1, 0)
    tcol = lax.broadcasted_iota(jnp.int32, (rows, block), 1)
    for s in range(hosts):
        limit = jnp.minimum(ibuf[s][:, 1:2] - start, count)
        tbias[pl.ds(s * rows, rows), :] = jnp.where(tcol < limit, 0.0, NEG).astype(jnp.float32)
    qt[...] = jnp.swapaxes(qbuf[...].reshape(total_rows, heads, -1), 0, 1)

    stat_m[...] = jnp.zeros_like(stat_m)
    stat_l[...] = jnp.zeros_like(stat_l)
    lane = lax.broadcasted_iota(jnp.int32, stat_m.shape, 1)

    def tail_head(h, _):
        own = pl.ds(ANCHOR, block)
        s = lax.dot_general(
            qt[h], kh[h, own, :], (((1,), (1,)), ((), ())), preferred_element_type=jnp.float32
        )
        s = s * scale + tbias[...]
        m = jnp.max(s, axis=-1, keepdims=True)
        w = jnp.exp2(s - m)
        stat_m[...] = jnp.where(lane == h, m, stat_m[...])
        stat_l[...] = jnp.where(lane == h, jnp.sum(w, axis=-1, keepdims=True), stat_l[...])
        high = w.astype(jnp.bfloat16)
        low = (w - high.astype(jnp.float32)).astype(jnp.bfloat16)
        v = vh[h, own, :]
        num = jnp.dot(high, v, preferred_element_type=jnp.float32)
        num = num + jnp.dot(low, v, preferred_element_type=jnp.float32)
        for d in range(hosts):
            psend[d, h] = num[d * rows : (d + 1) * rows].astype(jnp.bfloat16)
        return 0

    def head(h):
        s = lax.dot_general(
            qh[h], kh[h], (((1,), (1,)), ((), ())), preferred_element_type=jnp.float32
        )
        s = s * scale + bias[...]
        m = jnp.max(s, axis=-1, keepdims=True)
        w = jnp.exp2(s - m)
        den = jnp.sum(w, axis=-1, keepdims=True)
        o = jnp.dot(w.astype(jnp.bfloat16), vh[h], preferred_element_type=jnp.float32)
        oh[h] = (o / den).astype(jnp.bfloat16)

    def place(gl):
        for t in range(2):
            at = pl.ds((t * half + gl) * GROUP, GROUP)
            for i, dst in enumerate((kh, vh)):
                raw = a_raw[t, pl.ds(gl * per + i * PARTS, PARTS)]
                dst[at, pl.ds(0, ANCHOR), :] = jnp.swapaxes(
                    raw.reshape(ANCHOR, GROUP, raw.shape[-1]), 0, 1
                )

    def attend(gl, i):
        head((i // GROUP * half + gl) * GROUP + lax.rem(i, GROUP))

    def outs(gl):
        for t in range(2):
            g = t * half + gl
            yield g, pltpu.make_async_copy(
                o_raw.at[g], out_hbm.at[:, pl.ds(g * GROUP, GROUP), :], out_sem.at[g]
            )

    def finish(gl):
        for g, c in outs(gl):
            o_raw[g] = jnp.swapaxes(oh[pl.ds(g * GROUP, GROUP)], 0, 1)
            c.start()

    def p_copies(k):
        host = lax.rem(me + k, hosts)
        return (
            remote(psend.at[host], precv.at[me], p_send.at[k], p_recv.at[me], host),
            remote(ssend.at[host], srecv.at[me], s_send.at[k], s_recv.at[me], host),
        )

    def p_own():
        yield pltpu.make_async_copy(psend.at[me], precv.at[me], own_sem.at[0])
        yield pltpu.make_async_copy(ssend.at[me], srecv.at[me], own_sem.at[1])

    each = heads // per

    def step0(p, _):
        arrive(p)
        lax.fori_loop(0, each, lambda i, c: tail_head(p * each + i, c), 0)
        return 0

    lax.fori_loop(0, per, step0, 0)
    for d in range(hosts):
        ssend[d, 0] = stat_m[pl.ds(d * rows, rows), :]
        ssend[d, 1] = stat_l[pl.ds(d * rows, rows), :]
    place(0)

    for c in p_own():
        c.start()

    def send_part(k, _):
        for c in p_copies(k):
            c.start()
        return 0

    lax.fori_loop(1, hosts, send_part, 0)

    pairs = 2 * GROUP // per
    for gl in range(1, half):
        def step(p, _, gl=gl):
            arrive(gl * per + p)
            for i in range(pairs):
                attend(gl - 1, p * pairs + i)
            return 0

        lax.fori_loop(0, per, step, 0)
        finish(gl - 1)
        place(gl)

    def last(i, _):
        for j in range(2):
            attend(half - 1, i * 2 + j)
        return 0

    lax.fori_loop(0, GROUP, last, 0)
    finish(half - 1)

    for c in p_own():
        c.wait()

    def part_wait(k, _):
        s = lax.rem(me + k, hosts)
        remote(psend.at[s], precv.at[s], p_send.at[k], p_recv.at[s], me).wait_recv()
        remote(ssend.at[s], srecv.at[s], s_send.at[k], s_recv.at[s], me).wait_recv()
        return 0

    lax.fori_loop(1, hosts, part_wait, 0)
    peak = srecv[0, 0]
    for s in range(1, hosts):
        peak = jnp.maximum(peak, srecv[s, 0])
    total = jnp.zeros_like(peak)
    for s in range(hosts):
        total = total + jnp.exp2(srecv[s, 0] - peak) * srecv[s, 1]
    inverse = 1.0 / total
    acc[...] = jnp.zeros_like(acc)

    def merge(s, _):
        w = jnp.exp2(srecv[s, 0] - peak) * inverse
        for h in range(heads):
            acc[h] += w[:, h : h + 1] * precv[s, h].astype(jnp.float32)
        return 0

    lax.fori_loop(0, hosts, merge, 0)
    tail_ref[...] = jnp.swapaxes(acc[...], 0, 1).astype(jnp.bfloat16)

    for k in range(depth):
        for c in q_copies(k):
            c.wait_send()
    for k in range(1, depth):
        for c in q_forward(k):
            c.wait_send()

    def part_sent(k, _):
        for c in p_copies(k):
            c.wait_send()
        return 0

    lax.fori_loop(1, hosts, part_sent, 0)

    def sent(p, _):
        for t in range(2):
            for cond, copy in sends(t, p):
                @pl.when(cond)
                def _():
                    copy.wait_send()
        return 0

    lax.fori_loop(0, pieces, sent, 0)
    for gl in range(half):
        for _, c in outs(gl):
            c.wait()


def local(hosts, ctx_query, ctx_key, ctx_value, valid, tail_query, tail_position):
    block, heads, width = ctx_query.shape
    rows = tail_query.shape[0]
    groups = heads // GROUP
    pieces = groups // 2 * 2 * PARTS
    depth = hosts // 2
    lane = lax.broadcasted_iota(jnp.int32, (rows, 128), 1)
    info = jnp.where(lane == 0, valid[0], tail_position[:, None])
    bf, f32 = jnp.bfloat16, jnp.float32
    dma = pltpu.SemaphoreType.DMA
    anywhere = pl.BlockSpec(memory_space=pl.ANY)
    raw = pltpu.VMEM((groups, block, GROUP, width), bf)
    keys = pltpu.VMEM((heads, ANCHOR + block, width), bf)
    own = pltpu.VMEM((heads, block, width), bf)
    part = pltpu.VMEM((hosts, heads, rows, width), bf)
    stat = pltpu.VMEM((hosts, 2, rows, 128), f32)
    return pl.pallas_call(
        functools.partial(kernel, hosts, block, heads, rows),
        out_shape=(
            jax.ShapeDtypeStruct(ctx_query.shape, bf),
            jax.ShapeDtypeStruct(tail_query.shape, bf),
        ),
        in_specs=[anywhere] * 5,
        out_specs=(anywhere, pl.BlockSpec(memory_space=pltpu.VMEM)),
        scratch_shapes=[
            raw, raw, raw,
            pltpu.VMEM((2, pieces, ANCHOR // PARTS, GROUP, width), bf),
            own, keys, keys, own, raw,
            pltpu.VMEM((hosts, rows, heads, width), bf),
            pltpu.VMEM((hosts, rows, 128), jnp.int32),
            pltpu.VMEM((heads, hosts * rows, width), bf),
            pltpu.VMEM((block, ANCHOR + block), f32),
            pltpu.VMEM((hosts * rows, block), f32),
            pltpu.VMEM((hosts * rows, 128), f32),
            pltpu.VMEM((hosts * rows, 128), f32),
            part, part, stat, stat,
            pltpu.VMEM((heads, rows, width), f32),
            dma((3, groups)), dma((2, pieces)), dma((2,)), dma((groups,)),
            dma((2, pieces)), dma((2, 2, pieces)),
            dma((hosts,)), dma((hosts,)), dma((2 * depth,)), dma((2 * depth,)),
            dma((hosts,)), dma((hosts,)), dma((hosts,)), dma((hosts,)),
        ],
        compiler_params=pltpu.CompilerParams(
            collective_id=0, has_side_effects=True, vmem_limit_bytes=60 * 1024 * 1024
        ),
    )(ctx_query, ctx_key, ctx_value, tail_query, info)


def solution(mesh):
    wide = P(("groups", "hst"), "head", None)
    thin = P(("groups", "hst"))
    return jax.shard_map(
        functools.partial(local, mesh.shape["hst"]), mesh=mesh,
        in_specs=(wide, wide, wide, thin, wide, thin), out_specs=(wide, wide), check_vma=False,
    )
```

```python
import functools
import math

import jax
import jax.numpy as jnp
from jax import lax
from jax.experimental import pallas as pl
from jax.experimental.pallas import tpu as pltpu
from jax.sharding import PartitionSpec as P

ANCHOR = 128
GROUP = 8
LAG = 3
FLIGHT = 2
PARTS = 2
NEG = -1e30
MESH = pl.DeviceIdType.MESH


def kernel(
    hosts, block, heads, rows, q_hbm, k_hbm, v_hbm, tq_hbm, info_hbm, out_hbm, tail_ref,
    q_raw, k_raw, v_raw, a_raw, qh, kh, vh, oh, o_raw, qbuf, ibuf, qt, bias, tbias, stat_m, stat_l,
    psend, precv, ssend, srecv, acc,
    load_sem, root_sem, own_sem, out_sem, a_recv, a_send, q_recv, i_recv, q_send, i_send,
    p_recv, s_recv, p_send, s_send,
):
    depth = hosts // 2
    groups = heads // GROUP
    half = groups // 2
    piece_rows = ANCHOR // PARTS
    pieces = half * 2 * PARTS
    per = 2 * PARTS
    total_rows = hosts * rows
    scale = math.log2(math.e) / math.sqrt(q_hbm.shape[-1])
    me = lax.axis_index("hst")
    z, y = me // 2, lax.rem(me, 2)
    root = me == 0

    def remote(src, dst, ssem, rsem, host):
        return pltpu.make_async_remote_copy(
            src_ref=src, dst_ref=dst, send_sem=ssem, recv_sem=rsem,
            device_id={"hst": host}, device_id_type=MESH,
        )

    def loads():
        for i, (hbm, raw) in enumerate(((k_hbm, k_raw), (v_hbm, v_raw), (q_hbm, q_raw))):
            for g in range(groups):
                yield pltpu.make_async_copy(
                    hbm.at[:, pl.ds(g * GROUP, GROUP), :], raw.at[g], load_sem.at[i, g]
                )

    def root_loads():
        for t in range(2):
            for p in range(pieces):
                hbm = k_hbm if (p // PARTS) % 2 == 0 else v_hbm
                g = t * half + p // per
                yield pltpu.make_async_copy(
                    hbm.at[pl.ds((p % PARTS) * piece_rows, piece_rows), pl.ds(g * GROUP, GROUP), :],
                    a_raw.at[t, p], root_sem.at[t, p],
                )

    def own_loads():
        yield pltpu.make_async_copy(tq_hbm, qbuf.at[me], own_sem.at[0])
        yield pltpu.make_async_copy(info_hbm, ibuf.at[me], own_sem.at[1])

    @pl.when(root)
    def _():
        for c in root_loads():
            c.start()

    for c in own_loads():
        c.start()
    for c in loads():
        c.start()

    barrier = pltpu.get_barrier_semaphore()

    def greet(k, _):
        pl.semaphore_signal(
            barrier, inc=1, device_id={"hst": lax.rem(me + k, hosts)}, device_id_type=MESH
        )
        return 0

    lax.fori_loop(1, hosts, greet, 0)
    pl.semaphore_wait(barrier, hosts - 1)

    def q_first(k):
        if k == 0:
            return z * 2 + 1 - y
        return lax.rem(z + k, depth) * 2 + y

    def q_copies(k):
        host = q_first(k)
        return (
            remote(tq_hbm, qbuf.at[me], q_send.at[k], q_recv.at[me], host),
            remote(info_hbm, ibuf.at[me], i_send.at[k], i_recv.at[me], host),
        )

    def q_forward(k):
        slot = lax.rem(z + depth - k, depth) * 2 + y
        host = z * 2 + 1 - y
        return (
            remote(qbuf.at[slot], qbuf.at[slot], q_send.at[depth - 1 + k], q_recv.at[slot], host),
            remote(ibuf.at[slot], ibuf.at[slot], i_send.at[depth - 1 + k], i_recv.at[slot], host),
        )

    def q_wait(slot):
        remote(qbuf.at[slot], qbuf.at[slot], q_send.at[0], q_recv.at[slot], me).wait_recv()
        remote(ibuf.at[slot], ibuf.at[slot], i_send.at[0], i_recv.at[slot], me).wait_recv()

    for k in range(depth):
        for c in q_copies(k):
            c.start()

    def piece(t, p, ssem, host):
        return remote(a_raw.at[t, p], a_raw.at[t, p], ssem, a_recv.at[t, p], host)

    def main_sends(p):
        yield z + 1 < depth, piece(1 - y, p, a_send.at[0, p], me + 2)
        yield z >= 1, piece(1 - y, p, a_send.at[1, p], z * 2 + 1 - y)

    def other_sends(p):
        yield root, piece(y, p, a_send.at[2, p], 1)
        yield me == 3, piece(y, p, a_send.at[2, p], 1)

    def go(copies):
        for cond, copy in copies:
            @pl.when(cond)
            def _():
                copy.start()

    def root_sends(p):
        return piece(1 - y, p, a_send.at[0, p], me + 2), piece(y, p, a_send.at[2, p], 1)

    def main_step(p):
        if FLIGHT <= p:
            @pl.when(root)
            def _():
                for done, c in zip(root_sends(p - FLIGHT), root_sends(p)):
                    done.wait_send()
                    c.start()

        @pl.when(jnp.logical_not(root))
        def _():
            piece(1 - y, p, a_send.at[0, p], me).wait_recv()
            go(main_sends(p))

    def other_step(p, cond):
        @pl.when(cond)
        def _():
            piece(y, p, a_send.at[0, p], me).wait_recv()

            @pl.when(me == 3)
            def _():
                piece(y, p, a_send.at[2, p], 1).start()

    def step(p):
        if p < pieces:
            main_step(p)
        if LAG <= p < pieces + LAG:
            other_step(p - LAG, me > 1)
        if 2 * LAG <= p < pieces + 2 * LAG:
            other_step(p - 2 * LAG, me == 1)

    @pl.when(root)
    def _():
        for c in root_loads():
            c.wait()

        for p in range(FLIGHT):
            for c in root_sends(p):
                c.start()

    lane = lax.broadcasted_iota(jnp.int32, stat_m.shape, 1)

    def tail_head(h, _):
        own = pl.ds(ANCHOR, block)
        s = lax.dot_general(
            qt[h], kh[h, own, :], (((1,), (1,)), ((), ())), preferred_element_type=jnp.float32
        )
        s = s * scale + tbias[...]
        m = jnp.max(s, axis=-1, keepdims=True)
        w = jnp.exp2(s - m)
        stat_m[...] = jnp.where(lane == h, m, stat_m[...])
        stat_l[...] = jnp.where(lane == h, jnp.sum(w, axis=-1, keepdims=True), stat_l[...])
        high = w.astype(jnp.bfloat16)
        low = (w - high.astype(jnp.float32)).astype(jnp.bfloat16)
        v = vh[h, own, :]
        num = jnp.dot(high, v, preferred_element_type=jnp.float32)
        num = num + jnp.dot(low, v, preferred_element_type=jnp.float32)
        for d in range(hosts):
            psend[d, h] = num[d * rows : (d + 1) * rows].astype(jnp.bfloat16)
        return 0

    def head(h):
        s = lax.dot_general(
            qh[h], kh[h], (((1,), (1,)), ((), ())), preferred_element_type=jnp.float32
        )
        s = s * scale + bias[...]
        m = jnp.max(s, axis=-1, keepdims=True)
        w = jnp.exp2(s - m)
        den = jnp.sum(w, axis=-1, keepdims=True)
        o = jnp.dot(w.astype(jnp.bfloat16), vh[h], preferred_element_type=jnp.float32)
        oh[h] = (o / den).astype(jnp.bfloat16)

    def place(gl):
        for t in range(2):
            at = pl.ds((t * half + gl) * GROUP, GROUP)
            for i, dst in enumerate((kh, vh)):
                raw = a_raw[t, pl.ds(gl * per + i * PARTS, PARTS)]
                dst[at, pl.ds(0, ANCHOR), :] = jnp.swapaxes(
                    raw.reshape(ANCHOR, GROUP, raw.shape[-1]), 0, 1
                )

    def attend(gl, i):
        head((i // GROUP * half + gl) * GROUP + lax.rem(i, GROUP))

    def outs(gl):
        for t in range(2):
            g = t * half + gl
            yield g, pltpu.make_async_copy(
                o_raw.at[g], out_hbm.at[:, pl.ds(g * GROUP, GROUP), :], out_sem.at[g]
            )

    def finish(gl):
        for g, c in outs(gl):
            o_raw[g] = jnp.swapaxes(oh[pl.ds(g * GROUP, GROUP)], 0, 1)
            c.start()

    def p_copies(k):
        host = lax.rem(me + k, hosts)
        return (
            remote(psend.at[host], precv.at[me], p_send.at[k], p_recv.at[me], host),
            remote(ssend.at[host], srecv.at[me], s_send.at[k], s_recv.at[me], host),
        )

    def p_own():
        yield pltpu.make_async_copy(psend.at[me], precv.at[me], own_sem.at[0])
        yield pltpu.make_async_copy(ssend.at[me], srecv.at[me], own_sem.at[1])

    def load_wait(lo, hi):
        for i, c in enumerate(loads()):
            if lo * groups <= i < hi * groups:
                c.wait()

    def keys_item():
        load_wait(0, 2)

        def body(g, _):
            at = pl.ds(g * GROUP, GROUP)
            kh[at, pl.ds(ANCHOR, block), :] = jnp.swapaxes(k_raw[g], 0, 1)
            vh[at, pl.ds(ANCHOR, block), :] = jnp.swapaxes(v_raw[g], 0, 1)
            return 0

        lax.fori_loop(0, groups, body, 0)

    def query_item():
        load_wait(2, 3)

        def body(g, _):
            qh[pl.ds(g * GROUP, GROUP)] = jnp.swapaxes(q_raw[g], 0, 1)
            return 0

        lax.fori_loop(0, groups, body, 0)

    def bias_item():
        for c in own_loads():
            c.wait()
        count = ibuf[me][0:1, 0:1]
        keys = ANCHOR + block
        row = lax.broadcasted_iota(jnp.int32, (block, keys), 0)
        col = lax.broadcasted_iota(jnp.int32, (block, keys), 1)
        slot = col - ANCHOR
        own_bias = jnp.where((slot <= row) & (slot < count), jnp.float32(0.0), jnp.float32(NEG))
        bias[...] = jnp.where(slot < 0, jnp.where(root, jnp.float32(NEG), jnp.float32(0.0)), own_bias)
        stat_m[...] = jnp.zeros_like(stat_m)
        stat_l[...] = jnp.zeros_like(stat_l)

    def rows_item():
        for k in range(1, depth):
            q_wait(lax.rem(z + depth - k, depth) * 2 + y)
            for c in q_forward(k):
                c.start()

    def rows_done_item():
        count = ibuf[me][0:1, 0:1]
        for k in range(depth):
            q_wait(k * 2 + 1 - y)

        start = jnp.zeros((1, 1), jnp.int32)
        for s in range(hosts):
            start = start + ibuf[s][0:1, 0:1] * jnp.where(s < me, 1, 0)
        tcol = lax.broadcasted_iota(jnp.int32, (rows, block), 1)
        for s in range(hosts):
            limit = jnp.minimum(ibuf[s][:, 1:2] - start, count)
            tbias[pl.ds(s * rows, rows), :] = jnp.where(tcol < limit, 0.0, NEG).astype(jnp.float32)
        qt[...] = jnp.swapaxes(qbuf[...].reshape(total_rows, heads, -1), 0, 1)

    def tail_item(i):
        lax.fori_loop(i * 4, min(i * 4 + 4, heads), tail_head, 0)

    def send_item():
        for d in range(hosts):
            ssend[d, 0] = stat_m[pl.ds(d * rows, rows), :]
            ssend[d, 1] = stat_l[pl.ds(d * rows, rows), :]
        for c in p_own():
            c.start()
        lax.fori_loop(1, hosts, send_part, 0)

    def attend_item(gl, i):
        def body(j, _):
            for k in range(2):
                attend(gl, i * 4 + j * 2 + k)
            return 0

        lax.fori_loop(0, 2, body, 0)

    def send_part(k, _):
        for c in p_copies(k):
            c.start()
        return 0

    work = [keys_item, rows_item, bias_item, rows_done_item, query_item]
    work += [functools.partial(tail_item, i) for i in range(heads // 4)]
    work += [send_item]
    at = 0
    for item in work:
        step(at)
        at += 1
        item()
    for gl in range(half):
        need = (gl + 1) * per + 2 * LAG
        while at < need:
            step(at)
            at += 1
        place(gl)
        for i in range(2 * GROUP // 4):
            step(at)
            at += 1
            attend_item(gl, i)
        finish(gl)

    for c in p_own():
        c.wait()

    def part_wait(k, _):
        s = lax.rem(me + k, hosts)
        remote(psend.at[s], precv.at[s], p_send.at[k], p_recv.at[s], me).wait_recv()
        remote(ssend.at[s], srecv.at[s], s_send.at[k], s_recv.at[s], me).wait_recv()
        return 0

    lax.fori_loop(1, hosts, part_wait, 0)
    peak = srecv[0, 0]
    for s in range(1, hosts):
        peak = jnp.maximum(peak, srecv[s, 0])
    total = jnp.zeros_like(peak)
    for s in range(hosts):
        total = total + jnp.exp2(srecv[s, 0] - peak) * srecv[s, 1]
    inverse = 1.0 / total
    acc[...] = jnp.zeros_like(acc)

    def merge(s, _):
        w = jnp.exp2(srecv[s, 0] - peak) * inverse
        for h in range(heads):
            acc[h] += w[:, h : h + 1] * precv[s, h].astype(jnp.float32)
        return 0

    lax.fori_loop(0, hosts, merge, 0)
    tail_ref[...] = jnp.swapaxes(acc[...], 0, 1).astype(jnp.bfloat16)

    for k in range(depth):
        for c in q_copies(k):
            c.wait_send()
    for k in range(1, depth):
        for c in q_forward(k):
            c.wait_send()

    def part_sent(k, _):
        for c in p_copies(k):
            c.wait_send()
        return 0

    lax.fori_loop(1, hosts, part_sent, 0)

    def sent(p, _):
        for cond, copy in (*main_sends(p), *other_sends(p)):
            @pl.when(cond & (jnp.logical_not(root) | (p >= pieces - FLIGHT)))
            def _():
                copy.wait_send()
        return 0

    lax.fori_loop(0, pieces, sent, 0)
    for gl in range(half):
        for _, c in outs(gl):
            c.wait()


def local(hosts, ctx_query, ctx_key, ctx_value, valid, tail_query, tail_position):
    block, heads, width = ctx_query.shape
    rows = tail_query.shape[0]
    groups = heads // GROUP
    pieces = groups // 2 * 2 * PARTS
    depth = hosts // 2
    lane = lax.broadcasted_iota(jnp.int32, (rows, 128), 1)
    info = jnp.where(lane == 0, valid[0], tail_position[:, None])
    bf, f32 = jnp.bfloat16, jnp.float32
    dma = pltpu.SemaphoreType.DMA
    anywhere = pl.BlockSpec(memory_space=pl.ANY)
    raw = pltpu.VMEM((groups, block, GROUP, width), bf)
    keys = pltpu.VMEM((heads, ANCHOR + block, width), bf)
    own = pltpu.VMEM((heads, block, width), bf)
    part = pltpu.VMEM((hosts, heads, rows, width), bf)
    stat = pltpu.VMEM((hosts, 2, rows, 128), f32)
    return pl.pallas_call(
        functools.partial(kernel, hosts, block, heads, rows),
        out_shape=(
            jax.ShapeDtypeStruct(ctx_query.shape, bf),
            jax.ShapeDtypeStruct(tail_query.shape, bf),
        ),
        in_specs=[anywhere] * 5,
        out_specs=(anywhere, pl.BlockSpec(memory_space=pltpu.VMEM)),
        scratch_shapes=[
            raw, raw, raw,
            pltpu.VMEM((2, pieces, ANCHOR // PARTS, GROUP, width), bf),
            own, keys, keys, own, raw,
            pltpu.VMEM((hosts, rows, heads, width), bf),
            pltpu.VMEM((hosts, rows, 128), jnp.int32),
            pltpu.VMEM((heads, hosts * rows, width), bf),
            pltpu.VMEM((block, ANCHOR + block), f32),
            pltpu.VMEM((hosts * rows, block), f32),
            pltpu.VMEM((hosts * rows, 128), f32),
            pltpu.VMEM((hosts * rows, 128), f32),
            part, part, stat, stat,
            pltpu.VMEM((heads, rows, width), f32),
            dma((3, groups)), dma((2, pieces)), dma((2,)), dma((groups,)),
            dma((2, pieces)), dma((3, pieces)),
            dma((hosts,)), dma((hosts,)), dma((2 * depth,)), dma((2 * depth,)),
            dma((hosts,)), dma((hosts,)), dma((hosts,)), dma((hosts,)),
        ],
        compiler_params=pltpu.CompilerParams(
            collective_id=0, has_side_effects=True, vmem_limit_bytes=60 * 1024 * 1024
        ),
    )(ctx_query, ctx_key, ctx_value, tail_query, info)


def solution(mesh):
    wide = P(("groups", "hst"), "head", None)
    thin = P(("groups", "hst"))
    return jax.shard_map(
        functools.partial(local, mesh.shape["hst"]), mesh=mesh,
        in_specs=(wide, wide, wide, thin, wide, thin), out_specs=(wide, wide), check_vma=False,
    )
```

```python
import functools
import math

import jax
import jax.numpy as jnp
from jax import lax
from jax.experimental import pallas as pl
from jax.experimental.pallas import tpu as pltpu
from jax.sharding import PartitionSpec as P

ANCHOR = 128
GROUP = 8
LAG = 3
FLIGHT = 2
PARTS = 2
NEG = -1e30
MESH = pl.DeviceIdType.MESH


def kernel(
    hosts, block, heads, rows, q_hbm, k_hbm, v_hbm, tq_hbm, info_hbm, out_hbm, tail_ref,
    q_raw, k_raw, v_raw, a_raw, qh, kh, vh, oh, o_raw, qbuf, ibuf, qt, bias, tbias, stat_m, stat_l,
    psend, precv, ssend, srecv, acc,
    load_sem, root_sem, own_sem, out_sem, a_recv, a_send, q_recv, i_recv, q_send, i_send,
    p_recv, s_recv, p_send, s_send,
):
    depth = hosts // 2
    groups = heads // GROUP
    half = groups // 2
    piece_rows = ANCHOR // PARTS
    pieces = half * 2 * PARTS
    per = 2 * PARTS
    total_rows = hosts * rows
    scale = math.log2(math.e) / math.sqrt(q_hbm.shape[-1])
    me = lax.axis_index("hst")
    z, y = me // 2, lax.rem(me, 2)
    root = me == 0

    def remote(src, dst, ssem, rsem, host):
        return pltpu.make_async_remote_copy(
            src_ref=src, dst_ref=dst, send_sem=ssem, recv_sem=rsem,
            device_id={"hst": host}, device_id_type=MESH,
        )

    def loads():
        for i, (hbm, raw) in enumerate(((k_hbm, k_raw), (v_hbm, v_raw), (q_hbm, q_raw))):
            for g in range(groups):
                yield pltpu.make_async_copy(
                    hbm.at[:, pl.ds(g * GROUP, GROUP), :], raw.at[g], load_sem.at[i, g]
                )

    def root_loads():
        for t in range(2):
            for p in range(pieces):
                hbm = k_hbm if (p // PARTS) % 2 == 0 else v_hbm
                g = t * half + p // per
                yield pltpu.make_async_copy(
                    hbm.at[pl.ds((p % PARTS) * piece_rows, piece_rows), pl.ds(g * GROUP, GROUP), :],
                    a_raw.at[t, p], root_sem.at[t, p],
                )

    def own_loads():
        yield pltpu.make_async_copy(tq_hbm, qbuf.at[me], own_sem.at[0])
        yield pltpu.make_async_copy(info_hbm, ibuf.at[me], own_sem.at[1])

    @pl.when(root)
    def _():
        for c in root_loads():
            c.start()

    for c in own_loads():
        c.start()
    for c in loads():
        c.start()

    barrier = pltpu.get_barrier_semaphore()

    def greet(k, _):
        pl.semaphore_signal(
            barrier, inc=1, device_id={"hst": lax.rem(me + k, hosts)}, device_id_type=MESH
        )
        return 0

    lax.fori_loop(1, hosts, greet, 0)
    pl.semaphore_wait(barrier, hosts - 1)

    def q_first(k):
        if k == 0:
            return z * 2 + 1 - y
        return lax.rem(z + k, depth) * 2 + y

    def q_copies(k):
        host = q_first(k)
        return (
            remote(tq_hbm, qbuf.at[me], q_send.at[k], q_recv.at[me], host),
            remote(info_hbm, ibuf.at[me], i_send.at[k], i_recv.at[me], host),
        )

    def q_forward(k):
        slot = lax.rem(z + depth - k, depth) * 2 + y
        host = z * 2 + 1 - y
        return (
            remote(qbuf.at[slot], qbuf.at[slot], q_send.at[depth - 1 + k], q_recv.at[slot], host),
            remote(ibuf.at[slot], ibuf.at[slot], i_send.at[depth - 1 + k], i_recv.at[slot], host),
        )

    def q_wait(slot):
        remote(qbuf.at[slot], qbuf.at[slot], q_send.at[0], q_recv.at[slot], me).wait_recv()
        remote(ibuf.at[slot], ibuf.at[slot], i_send.at[0], i_recv.at[slot], me).wait_recv()

    for k in range(depth):
        for c in q_copies(k):
            c.start()

    def piece(t, p, ssem, host):
        return remote(a_raw.at[t, p], a_raw.at[t, p], ssem, a_recv.at[t, p], host)

    def main_sends(p):
        yield z + 1 < depth, piece(1 - y, p, a_send.at[0, p], me + 2)
        yield z >= 1, piece(1 - y, p, a_send.at[1, p], z * 2 + 1 - y)

    def other_sends(p):
        yield root, piece(y, p, a_send.at[2, p], 1)
        yield me == 3, piece(y, p, a_send.at[2, p], 1)

    def go(copies):
        for cond, copy in copies:
            @pl.when(cond)
            def _():
                copy.start()

    def root_sends(p):
        return piece(1 - y, p, a_send.at[0, p], me + 2), piece(y, p, a_send.at[2, p], 1)

    def main_step(p):
        if FLIGHT <= p:
            @pl.when(root)
            def _():
                for done, c in zip(root_sends(p - FLIGHT), root_sends(p)):
                    done.wait_send()
                    c.start()

        @pl.when(jnp.logical_not(root))
        def _():
            piece(1 - y, p, a_send.at[0, p], me).wait_recv()
            go(main_sends(p))

    def other_step(p, cond):
        @pl.when(cond)
        def _():
            piece(y, p, a_send.at[0, p], me).wait_recv()

            @pl.when(me == 3)
            def _():
                piece(y, p, a_send.at[2, p], 1).start()

    def step(p):
        if p < pieces:
            main_step(p)
        if LAG <= p < pieces + LAG:
            other_step(p - LAG, me > 1)
        if 2 * LAG <= p < pieces + 2 * LAG:
            other_step(p - 2 * LAG, me == 1)

    @pl.when(root)
    def _():
        for c in root_loads():
            c.wait()

        for p in range(FLIGHT):
            for c in root_sends(p):
                c.start()

    lane = lax.broadcasted_iota(jnp.int32, stat_m.shape, 1)

    def tail_head(h, _):
        own = pl.ds(ANCHOR, block)
        s = lax.dot_general(
            qt[h], kh[h, own, :], (((1,), (1,)), ((), ())), preferred_element_type=jnp.float32
        )
        s = s * scale + tbias[...]
        m = jnp.max(s, axis=-1, keepdims=True)
        w = jnp.exp2(s - m)
        stat_m[...] = jnp.where(lane == h, m, stat_m[...])
        stat_l[...] = jnp.where(lane == h, jnp.sum(w, axis=-1, keepdims=True), stat_l[...])
        high = w.astype(jnp.bfloat16)
        low = (w - high.astype(jnp.float32)).astype(jnp.bfloat16)
        v = vh[h, own, :]
        num = jnp.dot(high, v, preferred_element_type=jnp.float32)
        num = num + jnp.dot(low, v, preferred_element_type=jnp.float32)
        for d in range(hosts):
            psend[d, h] = num[d * rows : (d + 1) * rows].astype(jnp.bfloat16)
        return 0

    def head(h):
        s = lax.dot_general(
            qh[h], kh[h], (((1,), (1,)), ((), ())), preferred_element_type=jnp.float32
        )
        s = s * scale + bias[...]
        m = jnp.max(s, axis=-1, keepdims=True)
        w = jnp.exp2(s - m)
        den = jnp.sum(w, axis=-1, keepdims=True)
        o = jnp.dot(w.astype(jnp.bfloat16), vh[h], preferred_element_type=jnp.float32)
        oh[h] = (o / den).astype(jnp.bfloat16)

    def place(gl):
        for t in range(2):
            at = pl.ds((t * half + gl) * GROUP, GROUP)
            for i, dst in enumerate((kh, vh)):
                raw = a_raw[t, pl.ds(gl * per + i * PARTS, PARTS)]
                dst[at, pl.ds(0, ANCHOR), :] = jnp.swapaxes(
                    raw.reshape(ANCHOR, GROUP, raw.shape[-1]), 0, 1
                )

    def attend(gl, i):
        head((i // GROUP * half + gl) * GROUP + lax.rem(i, GROUP))

    def outs(gl):
        for t in range(2):
            g = t * half + gl
            yield g, pltpu.make_async_copy(
                o_raw.at[g], out_hbm.at[:, pl.ds(g * GROUP, GROUP), :], out_sem.at[g]
            )

    def finish(gl):
        for g, c in outs(gl):
            o_raw[g] = jnp.swapaxes(oh[pl.ds(g * GROUP, GROUP)], 0, 1)
            c.start()

    def p_copies(k):
        host = lax.rem(me + k, hosts)
        return (
            remote(psend.at[host], precv.at[me], p_send.at[k], p_recv.at[me], host),
            remote(ssend.at[host], srecv.at[me], s_send.at[k], s_recv.at[me], host),
        )

    def p_own():
        yield pltpu.make_async_copy(psend.at[me], precv.at[me], own_sem.at[0])
        yield pltpu.make_async_copy(ssend.at[me], srecv.at[me], own_sem.at[1])

    def load_wait(lo, hi):
        for i, c in enumerate(loads()):
            if lo * groups <= i < hi * groups:
                c.wait()

    def keys_item():
        load_wait(0, 2)

        def body(g, _):
            at = pl.ds(g * GROUP, GROUP)
            kh[at, pl.ds(ANCHOR, block), :] = jnp.swapaxes(k_raw[g], 0, 1)
            vh[at, pl.ds(ANCHOR, block), :] = jnp.swapaxes(v_raw[g], 0, 1)
            return 0

        lax.fori_loop(0, groups, body, 0)

    def query_item():
        load_wait(2, 3)

        def body(g, _):
            qh[pl.ds(g * GROUP, GROUP)] = jnp.swapaxes(q_raw[g], 0, 1)
            return 0

        lax.fori_loop(0, groups, body, 0)

    def bias_item():
        for c in own_loads():
            c.wait()
        count = ibuf[me][0:1, 0:1]
        keys = ANCHOR + block
        row = lax.broadcasted_iota(jnp.int32, (block, keys), 0)
        col = lax.broadcasted_iota(jnp.int32, (block, keys), 1)
        slot = col - ANCHOR
        own_bias = jnp.where((slot <= row) & (slot < count), jnp.float32(0.0), jnp.float32(NEG))
        bias[...] = jnp.where(slot < 0, jnp.where(root, jnp.float32(NEG), jnp.float32(0.0)), own_bias)
        stat_m[...] = jnp.zeros_like(stat_m)
        stat_l[...] = jnp.zeros_like(stat_l)

    def rows_item():
        for k in range(1, depth):
            q_wait(lax.rem(z + depth - k, depth) * 2 + y)
            for c in q_forward(k):
                c.start()

    def rows_done_item():
        count = ibuf[me][0:1, 0:1]
        for k in range(depth):
            q_wait(k * 2 + 1 - y)

        start = jnp.zeros((1, 1), jnp.int32)
        for s in range(hosts):
            start = start + ibuf[s][0:1, 0:1] * jnp.where(s < me, 1, 0)
        tcol = lax.broadcasted_iota(jnp.int32, (rows, block), 1)
        for s in range(hosts):
            limit = jnp.minimum(ibuf[s][:, 1:2] - start, count)
            tbias[pl.ds(s * rows, rows), :] = jnp.where(tcol < limit, 0.0, NEG).astype(jnp.float32)
        qt[...] = jnp.swapaxes(qbuf[...].reshape(total_rows, heads, -1), 0, 1)

    def tail_item(i):
        lax.fori_loop(i * 4, min(i * 4 + 4, heads), tail_head, 0, unroll=2)

    def send_item():
        for d in range(hosts):
            ssend[d, 0] = stat_m[pl.ds(d * rows, rows), :]
            ssend[d, 1] = stat_l[pl.ds(d * rows, rows), :]
        for c in p_own():
            c.start()
        lax.fori_loop(1, hosts, send_part, 0)

    def attend_item(gl, i):
        def body(j, _):
            for k in range(4):
                attend(gl, i * 4 + j * 4 + k)
            return 0

        lax.fori_loop(0, 1, body, 0)

    def send_part(k, _):
        for c in p_copies(k):
            c.start()
        return 0

    work = [keys_item, rows_item, bias_item, rows_done_item, query_item]
    work += [functools.partial(tail_item, i) for i in range(heads // 4)]
    work += [send_item]
    at = 0
    for item in work:
        step(at)
        at += 1
        item()
    for gl in range(half):
        need = (gl + 1) * per + 2 * LAG
        while at < need:
            step(at)
            at += 1
        place(gl)
        for i in range(2 * GROUP // 4):
            step(at)
            at += 1
            attend_item(gl, i)
        finish(gl)

    for c in p_own():
        c.wait()

    def part_wait(k, _):
        s = lax.rem(me + k, hosts)
        remote(psend.at[s], precv.at[s], p_send.at[k], p_recv.at[s], me).wait_recv()
        remote(ssend.at[s], srecv.at[s], s_send.at[k], s_recv.at[s], me).wait_recv()
        return 0

    lax.fori_loop(1, hosts, part_wait, 0)
    peak = srecv[0, 0]
    for s in range(1, hosts):
        peak = jnp.maximum(peak, srecv[s, 0])
    total = jnp.zeros_like(peak)
    for s in range(hosts):
        total = total + jnp.exp2(srecv[s, 0] - peak) * srecv[s, 1]
    inverse = 1.0 / total
    acc[...] = jnp.zeros_like(acc)

    def merge(s, _):
        w = jnp.exp2(srecv[s, 0] - peak) * inverse
        for h in range(heads):
            acc[h] += w[:, h : h + 1] * precv[s, h].astype(jnp.float32)
        return 0

    lax.fori_loop(0, hosts, merge, 0)
    tail_ref[...] = jnp.swapaxes(acc[...], 0, 1).astype(jnp.bfloat16)

    for k in range(depth):
        for c in q_copies(k):
            c.wait_send()
    for k in range(1, depth):
        for c in q_forward(k):
            c.wait_send()

    def part_sent(k, _):
        for c in p_copies(k):
            c.wait_send()
        return 0

    lax.fori_loop(1, hosts, part_sent, 0)

    def sent(p, _):
        for cond, copy in (*main_sends(p), *other_sends(p)):
            @pl.when(cond & (jnp.logical_not(root) | (p >= pieces - FLIGHT)))
            def _():
                copy.wait_send()
        return 0

    lax.fori_loop(0, pieces, sent, 0)
    for gl in range(half):
        for _, c in outs(gl):
            c.wait()


def local(hosts, ctx_query, ctx_key, ctx_value, valid, tail_query, tail_position):
    block, heads, width = ctx_query.shape
    rows = tail_query.shape[0]
    groups = heads // GROUP
    pieces = groups // 2 * 2 * PARTS
    depth = hosts // 2
    lane = lax.broadcasted_iota(jnp.int32, (rows, 128), 1)
    info = jnp.where(lane == 0, valid[0], tail_position[:, None])
    bf, f32 = jnp.bfloat16, jnp.float32
    dma = pltpu.SemaphoreType.DMA
    anywhere = pl.BlockSpec(memory_space=pl.ANY)
    raw = pltpu.VMEM((groups, block, GROUP, width), bf)
    keys = pltpu.VMEM((heads, ANCHOR + block, width), bf)
    own = pltpu.VMEM((heads, block, width), bf)
    part = pltpu.VMEM((hosts, heads, rows, width), bf)
    stat = pltpu.VMEM((hosts, 2, rows, 128), f32)
    return pl.pallas_call(
        functools.partial(kernel, hosts, block, heads, rows),
        out_shape=(
            jax.ShapeDtypeStruct(ctx_query.shape, bf),
            jax.ShapeDtypeStruct(tail_query.shape, bf),
        ),
        in_specs=[anywhere] * 5,
        out_specs=(anywhere, pl.BlockSpec(memory_space=pltpu.VMEM)),
        scratch_shapes=[
            raw, raw, raw,
            pltpu.VMEM((2, pieces, ANCHOR // PARTS, GROUP, width), bf),
            own, keys, keys, own, raw,
            pltpu.VMEM((hosts, rows, heads, width), bf),
            pltpu.VMEM((hosts, rows, 128), jnp.int32),
            pltpu.VMEM((heads, hosts * rows, width), bf),
            pltpu.VMEM((block, ANCHOR + block), f32),
            pltpu.VMEM((hosts * rows, block), f32),
            pltpu.VMEM((hosts * rows, 128), f32),
            pltpu.VMEM((hosts * rows, 128), f32),
            part, part, stat, stat,
            pltpu.VMEM((heads, rows, width), f32),
            dma((3, groups)), dma((2, pieces)), dma((2,)), dma((groups,)),
            dma((2, pieces)), dma((3, pieces)),
            dma((hosts,)), dma((hosts,)), dma((2 * depth,)), dma((2 * depth,)),
            dma((hosts,)), dma((hosts,)), dma((hosts,)), dma((hosts,)),
        ],
        compiler_params=pltpu.CompilerParams(
            collective_id=0, has_side_effects=True, vmem_limit_bytes=60 * 1024 * 1024
        ),
    )(ctx_query, ctx_key, ctx_value, tail_query, info)


def solution(mesh):
    wide = P(("groups", "hst"), "head", None)
    thin = P(("groups", "hst"))
    return jax.shard_map(
        functools.partial(local, mesh.shape["hst"]), mesh=mesh,
        in_specs=(wide, wide, wide, thin, wide, thin), out_specs=(wide, wide), check_vma=False,
    )
```
